32 devices in a mesh: dp: 1 (over z), tp: 32 (over y, x, core).
Axes of the slice: x: 4, y: 4, z: 1, core: 2. Of those that a mesh axis runs over, the one named last changes fastest.
The devices are a block of a 4x4x8 slice.
Arguments:
- hidden: bfloat16 [512, 4, 8192], P('dp')
- w_head: bfloat16 [8192, 32000], P(None, 'tp')
- q_draft: float32 [512, 3, 32000], P(('dp', 'tp'))
- x_draft: int32 [512, 3], P('dp')
Outputs:
- output 1: float32 [512, 3], P(('dp', 'tp'))
- output 2: float32 [512], P(('dp', 'tp'))
- output 3: float32 [512, 3, 32000], P(('dp', 'tp'))
- output 4: float32 [512, 32000], P(('dp', 'tp'))
All inputs are finite; a program needn't handle non-finite values.
Results may differ from the reference program's by a relative error of at most 0.001.
Values are sent between devices in bfloat16 or wider.
A program may use at most 768 MiB of HBM per device.

```python
import jax
import jax.numpy as jnp
from jax import lax

BATCH = 512
DRAFT = 3
HIDDEN = 8192
VOCAB = 32000
INV_TEMP = 1.25


def draw_tokens(token_key):
    tokens = jax.random.randint(token_key, (BATCH, DRAFT), 0, VOCAB, dtype=jnp.int32)
    return tokens.at[0, 0].set(VOCAB - 1).at[0, 1].set(0)


def setup_inputs(seed: int = 0, part: int = 0) -> dict:
    root_key = jax.random.key(seed)
    shared_key, part_root = jax.random.split(root_key)
    part_key = jax.random.fold_in(part_root, part)
    key_hidden, key_draft, key_token = jax.random.split(part_key, 3)
    raw_hidden = jax.random.normal(key_hidden, (BATCH, DRAFT + 1, HIDDEN), jnp.float32)
    hidden = raw_hidden * lax.rsqrt(jnp.mean(raw_hidden * raw_hidden, axis=-1, keepdims=True) + 1e-6)
    w_head = jax.random.normal(shared_key, (HIDDEN, VOCAB), jnp.float32) * HIDDEN ** -0.5
    draft_logits = 1.25 * jax.random.normal(key_draft, (BATCH, DRAFT, VOCAB), jnp.float32)
    q_draft = jax.nn.softmax(draft_logits, axis=-1)
    return {"hidden": hidden.astype(jnp.bfloat16), "w_head": w_head.astype(jnp.bfloat16), "q_draft": q_draft, "x_draft": draw_tokens(key_token)}


def reference(hidden, w_head, q_draft, x_draft):
    def verify_one(seq_args):
        hidden_seq, q_seq, x_seq = seq_args
        logits = jnp.dot(hidden_seq, w_head, preferred_element_type=jnp.float32) * INV_TEMP
        row_peak = jnp.max(logits, axis=-1, keepdims=True)
        exp_vals = jnp.exp(logits - row_peak)
        target_p = exp_vals / jnp.sum(exp_vals, axis=-1, keepdims=True)
        draft_p = target_p[:DRAFT]
        p_pick = jnp.take_along_axis(draft_p, x_seq[:, None], axis=1)[:, 0]
        q_pick = jnp.take_along_axis(q_seq, x_seq[:, None], axis=1)[:, 0]
        seq_accept = jnp.minimum(1.0, p_pick / q_pick)
        seq_expected = jnp.sum(jnp.cumprod(seq_accept))
        excess = jnp.maximum(draft_p - q_seq, 0.0)
        seq_resid = excess / jnp.sum(excess, axis=-1, keepdims=True)
        return seq_accept, seq_expected, seq_resid, target_p[DRAFT]

    accept, expected, residual, bonus = lax.map(verify_one, (hidden, q_draft, x_draft))
    return accept, expected, residual, bonus
```

```python
import functools
import math

import jax
import jax.numpy as jnp
from jax import lax
from jax.experimental import pallas as pl
from jax.experimental.pallas import tpu as pltpu
from jax.sharding import PartitionSpec as P

INV_TEMP = 1.25
LANES = 128
TOP_CODE = 65535.0
MAX_SPAN = 87.0
LOG2E = math.log2(math.e)


def chip_order(side):
    offsets = [(dy, dx) for dy in range(side) for dx in range(side)]
    back = lambda o: (-o[0] % side, -o[1] % side)
    reach = lambda o: min(o[0], side - o[0]) + min(o[1], side - o[1])
    two_way = sorted((o for o in offsets if o < back(o)), key=lambda o: (-reach(o), o))
    one_way = sorted((o for o in offsets if o == back(o)), key=lambda o: -reach(o))
    pairs = [(o, back(o)) for o in two_way]
    pairs += [(one_way[i], one_way[i + 1]) for i in range(0, len(one_way), 2)]
    return pairs


def logits_kernel(n, tp, h_ref, w_ref, code_ref, stat_ref, wbuf, hbuf, acc, sbuf, stcol, stbuf,
                  wsem, hsem, code_send, code_recv, stat_send, stat_recv, self_sem):
    cores = 2
    side = math.isqrt(n // cores)
    pairs = chip_order(side)
    n_steps = len(pairs)
    me = lax.axis_index(tp)
    my_chip = me // cores
    my_y, my_x = my_chip // side, my_chip % side
    cols, depth = w_ref.shape
    half = code_ref.shape[2]
    seqs, tiles, pos, _ = h_ref.shape
    chip_seqs = seqs // (n // cores)
    dev_rows = chip_seqs // cores * pos
    blk_seqs = dev_rows // pos
    rows = 2 * chip_seqs * pos
    slices = wsem.shape[0]
    span = tiles // slices

    def chip_at(dy, dx):
        return ((my_y + dy) % side) * side + (my_x + dx) % side

    def pack(column):
        total = 0
        for value in reversed(column):
            total = total * side + value
        return total

    tables = tuple(pack([pair[a][b] for pair in pairs]) for a in range(2) for b in range(2))

    def fetch(slot, k, chips):
        for a in range(2):
            pltpu.make_async_copy(
                h_ref.at[pl.ds(chips[a] * chip_seqs, chip_seqs), pl.ds(k * span, span)],
                hbuf.at[slot, pl.ds(a * chip_seqs, chip_seqs), pl.ds(k * span, span)],
                hsem.at[slot, k]).start()

    first = tuple(chip_at(*pairs[0][a]) for a in range(2))
    for k in range(slices):
        cut = pl.ds(k * span * LANES, span * LANES)
        pltpu.make_async_copy(w_ref.at[:, cut], wbuf.at[:, cut], wsem.at[k]).start()
        fetch(0, k, first)

    barrier = pltpu.get_barrier_semaphore()

    def tell(i, carry):
        pl.semaphore_signal(barrier, inc=1, device_id={tp: (me + i) % n},
                            device_id_type=pl.DeviceIdType.MESH)
        return carry

    lax.fori_loop(1, n, tell, 0)
    pl.semaphore_wait(barrier, n - 1)

    col_tiles = acc.shape[0]
    tail = [min(LANES, cols - t * LANES) for t in range(col_tiles)]
    acc[...] = jnp.zeros_like(acc)

    def one_pair(i, carry):
        digits = carry
        slot = i % 2
        chips = tuple(chip_at(digits[2 * a] % side, digits[2 * a + 1] % side) for a in range(2))
        digits = tuple(d // side for d in digits)

        @pl.when(i + 1 < n_steps)
        def _():
            coming = tuple(chip_at(digits[2 * a] % side, digits[2 * a + 1] % side) for a in range(2))
            for k in range(slices):
                fetch(1 - slot, k, coming)

        def one_slice(k, c):
            pltpu.make_async_copy(hbuf.at[slot, :, pl.ds(0, span)], hbuf.at[slot, :, pl.ds(0, span)],
                                  hsem.at[slot, k]).wait()

            @pl.when(i == 0)
            def _():
                cut = pl.ds(0, span * LANES)
                pltpu.make_async_copy(wbuf.at[:, cut], wbuf.at[:, cut], wsem.at[k]).wait()

            x = jnp.concatenate([hbuf[slot, :, k * span + u].reshape(rows, LANES) for u in range(span)], axis=1)
            w = wbuf[:, pl.ds(pl.multiple_of(k * span * LANES, span * LANES), span * LANES)]
            z = lax.dot_general(x, w, (((1,), (1,)), ((), ())), preferred_element_type=jnp.float32)
            for t in range(col_tiles):
                acc[t, :, :tail[t]] += z[:, t * LANES:t * LANES + tail[t]]
            return c

        lax.fori_loop(0, slices, one_slice, 0)

        def code_rows(d, c):
            for j in range(pos):
                z = jnp.concatenate([acc[t, pl.ds(d * dev_rows + j, blk_seqs, stride=pos), :]
                                     for t in range(col_tiles)], axis=1) * INV_TEMP
                live = z[:, :cols]
                peak = jnp.max(live, axis=1, keepdims=True)
                low = jnp.min(live, axis=1, keepdims=True)
                width = jnp.clip(peak - low, 1e-30, MAX_SPAN)
                mass = jnp.sum(jnp.exp(live - peak), axis=1, keepdims=True)
                code = jnp.clip((peak - z) * (TOP_CODE / width), 0.0, TOP_CODE) + 0.5
                code = code.astype(jnp.int32)
                sbuf[i * 2 * cores + d, j * blk_seqs:(j + 1) * blk_seqs, :] = (
                    code[:, :half] | (code[:, half:] << 16))
                lane = lax.broadcasted_iota(jnp.int32, (blk_seqs, LANES), 1)
                stat = jnp.where(lane == 0, peak, jnp.where(lane == 1, width * (1.0 / TOP_CODE), mass))
                stcol[pl.ds(pl.multiple_of(d * dev_rows + j * blk_seqs, blk_seqs), blk_seqs), :] = stat
            return c

        lax.fori_loop(0, 2 * cores, code_rows, 0)
        acc[...] = jnp.zeros_like(acc)
        for a in range(2):
            flat = stcol[a * LANES:(a + 1) * LANES, :].T
            stbuf[2 * i + a] = flat[:8]

        for d in range(2 * cores):
            dest = chips[d // cores] * cores + d % cores
            src = sbuf.at[i * 2 * cores + d]
            stat_src = stbuf.at[2 * i + d // cores]

            @pl.when(dest == me)
            def _():
                pltpu.make_async_copy(src, code_ref.at[me], self_sem.at[0]).start()
                pltpu.make_async_copy(stat_src, stat_ref.at[me], self_sem.at[1]).start()

            @pl.when(dest != me)
            def _():
                pltpu.make_async_remote_copy(src, code_ref.at[me], code_send, code_recv, device_id={tp: dest},
                                             device_id_type=pl.DeviceIdType.MESH).start()
                pltpu.make_async_remote_copy(stat_src, stat_ref.at[me], stat_send, stat_recv, device_id={tp: dest},
                                             device_id_type=pl.DeviceIdType.MESH).start()

        return digits

    lax.fori_loop(0, n_steps, one_pair, tuple(jnp.int32(t) for t in tables))

    others = pl.ds(0, n - 1)
    pltpu.make_async_copy(code_ref.at[0], code_ref.at[0], self_sem.at[0]).wait()
    pltpu.make_async_copy(stat_ref.at[0], stat_ref.at[0], self_sem.at[1]).wait()
    for sem in (code_send, code_recv):
        pltpu.make_async_copy(code_ref.at[others], code_ref.at[others], sem).wait()
    for sem in (stat_send, stat_recv):
        pltpu.make_async_copy(stat_ref.at[others], stat_ref.at[others], sem).wait()


def exchange_logits(n, tp, hidden, w_shard):
    seqs, pos, depth = hidden.shape
    cols = w_shard.shape[1]
    tiles = depth // LANES
    half = pl.cdiv(cols, 2 * LANES) * LANES
    dev_rows = seqs // n * pos
    slices = 4
    h_tiles = hidden.reshape(seqs, pos, tiles, LANES).transpose(0, 2, 1, 3)
    blk = 4 * dev_rows
    return pl.pallas_call(
        functools.partial(logits_kernel, n, tp),
        out_shape=(jax.ShapeDtypeStruct((n, dev_rows, half), jnp.int32),
                   jax.ShapeDtypeStruct((n, 8, LANES), jnp.float32)),
        in_specs=[pl.BlockSpec(memory_space=pl.ANY)] * 2,
        out_specs=(pl.BlockSpec(memory_space=pl.ANY),) * 2,
        scratch_shapes=[
            pltpu.VMEM((cols, depth), jnp.bfloat16),
            pltpu.VMEM((2, blk // pos, tiles, pos, LANES), jnp.bfloat16),
            pltpu.VMEM((2 * half // LANES, blk, LANES), jnp.float32),
            pltpu.VMEM((n, dev_rows, half), jnp.int32),
            pltpu.VMEM((blk, LANES), jnp.float32),
            pltpu.VMEM((n // 2, 8, LANES), jnp.float32),
            pltpu.SemaphoreType.DMA((slices,)),
            pltpu.SemaphoreType.DMA((2, slices)),
            pltpu.SemaphoreType.DMA,
            pltpu.SemaphoreType.DMA,
            pltpu.SemaphoreType.DMA,
            pltpu.SemaphoreType.DMA,
            pltpu.SemaphoreType.DMA((2,)),
        ],
        compiler_params=pltpu.CompilerParams(collective_id=0, has_side_effects=True,
                                             vmem_limit_bytes=40 * 1024 * 1024),
        cost_estimate=pl.CostEstimate(flops=2 * seqs * pos * depth * cols,
                                      bytes_accessed=2 * (seqs * pos * depth + depth * cols), transcendentals=0),
        name="logits_exchange",
    )(h_tiles, w_shard.T)


def verify_kernel(n, tp, draft, code_ref, stat_ref, q_ref, x_ref, resid_ref, bonus_ref, accept_ref, expect_ref,
                  scale, prob, picks):
    g = pl.program_id(0)
    halves = prob_rows = 2
    me = lax.axis_index(tp)
    cols = prob.shape[1] // n
    half = code_ref.shape[2]
    own = code_ref.shape[1]
    width = prob.shape[1]
    lane = lax.broadcasted_iota(jnp.int32, (own, LANES), 1)
    sub = lax.broadcasted_iota(jnp.int32, (own, LANES), 0)

    @pl.when(g == 0)
    def _():
        mine = (me % 2) * (LANES // 2)
        turn = (LANES - mine) % LANES
        peak = pltpu.roll(stat_ref[:, 0, :], turn, 1)
        step = pltpu.roll(stat_ref[:, 1, :], turn, 1)
        mass = pltpu.roll(stat_ref[:, 2, :], turn, 1)
        top = jnp.max(peak, axis=0, keepdims=True)
        total = jnp.sum(mass * jnp.exp(peak - top), axis=0, keepdims=True)
        slope = step * (-LOG2E)
        base = (peak - top) * LOG2E - jnp.log(total) * LOG2E
        pad = jnp.zeros((LANES - 2 * n, LANES), jnp.float32)
        scale[...] = jnp.concatenate([slope, base, pad], axis=0).T
        picks[...] = jnp.zeros_like(picks)

    order = (g + (draft * halves)) % ((draft + 1) * halves)
    j = order // halves
    hb = order % halves
    row = scale[pl.ds(pl.multiple_of(order * own, own), own), :]
    for s in range(n):
        word = code_ref[s]
        low = (word & 0xFFFF).astype(jnp.float32)
        high = lax.shift_right_logical(word, 16).astype(jnp.float32)
        slope = row[:, s:s + 1]
        base = row[:, n + s:n + s + 1]
        both = jnp.concatenate([low, high], axis=1)
        prob[:, s * cols:(s + 1) * cols] = jnp.exp2(both * slope + base)[:, :cols]

    parts = 25
    part = width // parts

    @pl.when(j == draft)
    def _():
        def move(t, c):
            at = pl.ds(pl.multiple_of(t * part, LANES), part)
            bonus_ref[:, at] = prob[:, at]
            return c
        lax.fori_loop(0, parts, move, 0)

    @pl.when(j != draft)
    def _():
        names = jnp.broadcast_to(x_ref[pl.ds(j, 1), :], (own, x_ref.shape[1]))
        at_row = lax.broadcasted_iota(jnp.int32, names.shape, 1) == (
            lax.broadcasted_iota(jnp.int32, names.shape, 0) + me * (halves * own) + hb * own)
        name = jnp.sum(jnp.where(at_row, names, 0), axis=1, keepdims=True)
        wanted = name - lane

        def weigh(t, c):
            total, p_pick, q_pick = c
            for u in range(part // LANES):
                start = pl.multiple_of(t * part + u * LANES, LANES)
                p = prob[:, pl.ds(start, LANES)]
                q = q_ref[0, :, pl.ds(start, LANES)]
                over = jnp.maximum(p - q, 0.0)
                resid_ref[0, :, pl.ds(start, LANES)] = over
                total = total + over
                hit = wanted == start
                p_pick = jnp.where(hit, p, p_pick)
                q_pick = jnp.where(hit, q, q_pick)
            return total, p_pick, q_pick

        zero = jnp.zeros((own, LANES), jnp.float32)
        total, p_pick, q_pick = lax.fori_loop(0, parts, weigh, (zero, zero, zero))
        share = 1.0 / jnp.sum(total, axis=1, keepdims=True)

        def rescale(t, c):
            at = pl.ds(pl.multiple_of(t * part, LANES), part)
            resid_ref[0, :, at] = resid_ref[0, :, at] * share
            return c
        lax.fori_loop(0, parts, rescale, 0)

        ratio = jnp.sum(p_pick, axis=1, keepdims=True) / jnp.sum(q_pick, axis=1, keepdims=True)
        taken = jnp.minimum(1.0, ratio)
        spread = jnp.sum(jnp.where(lane == sub + hb * own, taken, 0.0), axis=0, keepdims=True)
        picks[pl.ds(j, 1), :] = picks[pl.ds(j, 1), :] + spread

    @pl.when(g == pl.num_programs(0) - 1)
    def _():
        run = jnp.ones((1, LANES), jnp.float32)
        tally = jnp.zeros((1, LANES), jnp.float32)
        for d in range(draft):
            run = run * picks[d:d + 1, :]
            tally = tally + run
        accept_ref[...] = picks[:draft, :halves * own]
        expect_ref[...] = tally[:, :halves * own]


def verify(n, tp, codes, stats, q_rows, x_group):
    seq_dev, draft, vocab = q_rows.shape
    half = codes.shape[2]
    own = 8
    halves = seq_dev // own
    q_by_pos = q_rows.transpose(1, 0, 2)
    x_by_pos = x_group.T
    last = (draft + 1) * halves
    spot = lambda g: (g + draft * halves) % last
    at_draft = lambda g: jnp.maximum(g - halves, 0)
    resid, bonus, accept, expect = pl.pallas_call(
        functools.partial(verify_kernel, n, tp, draft),
        grid=(last,),
        out_shape=(jax.ShapeDtypeStruct((draft, seq_dev, vocab), jnp.float32),
                   jax.ShapeDtypeStruct((seq_dev, vocab), jnp.float32),
                   jax.ShapeDtypeStruct((draft, seq_dev), jnp.float32),
                   jax.ShapeDtypeStruct((1, seq_dev), jnp.float32)),
        in_specs=[pl.BlockSpec((n, own, half), lambda g: (0, spot(g), 0)),
                  pl.BlockSpec(stats.shape, lambda g: (0, 0, 0)),
                  pl.BlockSpec((1, own, vocab), lambda g: (at_draft(g) // halves, at_draft(g) % halves, 0)),
                  pl.BlockSpec(x_by_pos.shape, lambda g: (0, 0))],
        out_specs=(pl.BlockSpec((1, own, vocab), lambda g: (at_draft(g) // halves, at_draft(g) % halves, 0)),
                   pl.BlockSpec((own, vocab), lambda g: (jnp.minimum(g, halves - 1), 0)),
                   pl.BlockSpec((draft, seq_dev), lambda g: (0, 0)),
                   pl.BlockSpec((1, seq_dev), lambda g: (0, 0))),
        scratch_shapes=[pltpu.VMEM((LANES, LANES), jnp.float32),
                        pltpu.VMEM((own, vocab), jnp.float32),
                        pltpu.VMEM((8, LANES), jnp.float32)],
        compiler_params=pltpu.CompilerParams(dimension_semantics=("arbitrary",),
                                             vmem_limit_bytes=32 * 1024 * 1024),
        name="verify_rows",
    )(codes, stats, q_by_pos, x_by_pos)
    return accept.T, expect[0], resid.transpose(1, 0, 2), bonus


def solution(mesh):
    n = mesh.shape["tp"]

    def local_step(hidden, w_shard, q_rows, x_group):
        codes, stats = exchange_logits(n, "tp", hidden, w_shard)
        return verify(n, "tp", codes, stats, q_rows, x_group)

    return jax.shard_map(local_step, mesh=mesh,
                         in_specs=(P("dp", None, None), P(None, "tp"), P(("dp", "tp"), None, None), P("dp", None)),
                         out_specs=(P(("dp", "tp"), None), P(("dp", "tp")), P(("dp", "tp"), None, None), P(("dp", "tp"), None)),
                         check_vma=False)
```
